32 devices in a mesh: rep: 4 (over x, y), dp: 8 (over z, core).
Axes of the slice: x: 2, y: 2, z: 4, core: 2. Of those that a mesh axis runs over, the one named last changes fastest.
Arguments:
- x: bfloat16 [32, 4096, 896], P(('rep', 'dp')), parts along dimension 0
- dy: bfloat16 [32, 4096, 896], P(('rep', 'dp')), parts along dimension 0
- w_gate: bfloat16 [2, 896, 2560], P(None, 'dp')
- w_up: bfloat16 [2, 896, 2560], P(None, 'dp')
- w_down: bfloat16 [2, 2560, 896], P(None, 'dp')
Outputs:
- output 1: bfloat16 [32, 4096, 896], P(('rep', 'dp')), parts along dimension 0
- output 2: bfloat16 [8, 896, 2560], P('rep', 'dp'), parts along dimension 0
- output 3: bfloat16 [8, 896, 2560], P('rep', 'dp'), parts along dimension 0
- output 4: bfloat16 [8, 2560, 896], P('rep', 'dp'), parts along dimension 0
There are 4 independent parts. The reference program is written for one: setup_inputs(seed, part) draws one part's arguments, and reference() takes and returns one part's arrays. A program takes and returns all parts, laid end to end along the dimension named above; an argument that names none is the same for every part.
All inputs are finite; a program needn't handle non-finite values.
Results may differ from the reference program's by a relative error of at most 0.018.
Values are sent between devices in bfloat16 or wider.
A program may use at most 2 GiB of HBM per device.

```python
import jax
import jax.numpy as jnp
from jax import lax

SEQUENCES = 8
TOKENS = 4096
D = 896
FF = 2560
LAYERS = 2
NAMES = ("w_gate", "w_up", "w_down")
SHAPES = {"w_gate": (LAYERS, D, FF), "w_up": (LAYERS, D, FF), "w_down": (LAYERS, FF, D)}


def bump(key, n, height):
    away = (jnp.arange(n, dtype=jnp.int32) - jax.random.randint(key, (), 0, n, jnp.int32)) % n
    return jnp.where(away < n // 8, height, 1.0)


def together(key, own, strength):
    shared = jax.random.normal(key, own.shape[1:], jnp.float32)
    return (own + strength * shared) * lax.rsqrt(1 + strength * strength)


def setup_inputs(seed: int = 0, part: int = 0) -> dict:
    kx, kdy, ka, kb, kz, kf, kh, kl, *kw = jax.random.split(jax.random.key(seed), 8 + len(NAMES))
    kx, kdy, ka, kb = (jax.random.fold_in(k, part) for k in (kx, kdy, ka, kb))
    shape = (SEQUENCES, TOKENS, D)
    much_x, much_dy = jax.random.uniform(kz, (2,), jnp.float32, 0.0, 1.0)
    layers = 2.0 ** jax.random.uniform(kl, (LAYERS, 1, 1), jnp.float32, -1.0, 1.0)
    x = together(ka, jax.random.normal(kx, shape, jnp.float32), much_x) * bump(kf, D, 4.0)
    dy = together(kb, jax.random.normal(kdy, shape, jnp.float32), much_dy)
    drawn = {"x": x.astype(jnp.bfloat16), "dy": (dy * (SEQUENCES * TOKENS) ** -0.5).astype(jnp.bfloat16)}
    for key, name in zip(kw, NAMES, strict=True):
        w = jax.random.normal(key, SHAPES[name], jnp.float32) * SHAPES[name][1] ** -0.5
        drawn[name] = (w * {"w_gate": 1.0, "w_up": bump(kh, FF, 4.0), "w_down": layers}[name]).astype(jnp.bfloat16)
    return drawn


def matmul(a, w):
    return jnp.dot(a, w, preferred_element_type=jnp.float32).astype(jnp.bfloat16)


def normed(h):
    wide = h.astype(jnp.float32)
    scale = lax.rsqrt(jnp.mean(wide**2, -1, keepdims=True) + 1e-6)
    return (wide * scale).astype(jnp.bfloat16)


def layer(h, w):
    a = normed(h)
    gate = jnp.dot(a, w["w_gate"], preferred_element_type=jnp.float32)
    up = jnp.dot(a, w["w_up"], preferred_element_type=jnp.float32)
    return h + matmul((jax.nn.silu(gate) * up).astype(jnp.bfloat16), w["w_down"])


def stack(weights, h):
    return lax.scan(lambda h, w: (layer(h, w), None), h, weights)[0]


def reference(x, dy, w_gate, w_up, w_down):
    weights = dict(zip(NAMES, (w_gate, w_up, w_down), strict=True))

    def take(so_far, sequence):
        h, by_y = sequence
        _, back = jax.vjp(stack, weights, h)
        by_weights, by_h = back(by_y)
        return jax.tree.map(lambda total, term: total + term.astype(jnp.float32), so_far, by_weights), by_h

    none_yet = {name: jnp.zeros(w.shape, jnp.float32) for name, w in weights.items()}
    by_weights, by_x = lax.scan(take, none_yet, (x, dy))
    return (by_x, *(by_weights[name].astype(jnp.bfloat16) for name in NAMES))
```

```python
import functools

import jax
import jax.numpy as jnp
from jax import lax
from jax.experimental import pallas as pl
from jax.experimental.pallas import tpu as pltpu
from jax.sharding import PartitionSpec as P

MESH = pl.DeviceIdType.MESH
F32, BF16 = jnp.float32, jnp.bfloat16
NC = 10
VMEM = 67_000_000
TILE = 512
WIDE = 1024


def dot(a, b):
    return jnp.dot(a, b, preferred_element_type=F32)


def dot_nt(a, b):
    return lax.dot_general(a, b, (((1,), (1,)), ((), ())), preferred_element_type=F32)


def sigmoid(x):
    return 0.5 * jnp.tanh(0.5 * x) + 0.5


def forward_kernel(a, wg, wu, wd, out, acc, wgt, wut, wdt):
    step = pl.program_id(0)
    c = wgt.shape[0]
    tokens = a.shape[1]
    wgt[...] = wg[0].T
    wut[...] = wu[0].T
    wdt[...] = wd[0].reshape(c, a.shape[0]).T

    @pl.when(step == 0)
    def _():
        acc[...] = jnp.zeros_like(acc)

    def body(t, _):
        for k in range(2):
            at = pl.ds(pl.multiple_of((2 * t + k) * TILE, TILE), TILE)
            x = a[:, at]
            gate, up = dot(wgt[...], x), dot(wut[...], x)
            hid = (gate * sigmoid(gate) * up).astype(BF16)
            acc[:, at] += dot(wdt[...], hid)
        return 0

    lax.fori_loop(0, tokens // TILE // 2, body, 0)

    @pl.when(step == NC - 1)
    def _():
        out[...] = acc[...].astype(BF16)


def weight_specs(d, c):
    at = lambda s: jnp.minimum(s, NC - 1)
    cols = pl.BlockSpec((1, d, c), lambda s: (at(s) // 2, 0, at(s) % 2))
    rows = pl.BlockSpec((1, 8, c // 8, d), lambda s: (at(s) // 2, 0, at(s) % 2, 0))
    return [cols, cols, rows]


def forward(a, wg, wu, wd):
    d, tokens = a.shape
    c = wg.shape[2] // 2
    whole = pl.BlockSpec((d, tokens), lambda s: (0, 0), pipeline_mode=pl.Buffered(1))
    flops = 6 * d * tokens * c * NC
    return pl.pallas_call(
        forward_kernel,
        grid=(NC,),
        out_shape=jax.ShapeDtypeStruct((d, tokens), BF16),
        in_specs=[whole, *weight_specs(d, c)],
        out_specs=whole,
        scratch_shapes=[
            pltpu.VMEM((d, tokens), F32),
            pltpu.VMEM((c, d), BF16),
            pltpu.VMEM((c, d), BF16),
            pltpu.VMEM((d, c), BF16),
        ],
        compiler_params=pltpu.CompilerParams(vmem_limit_bytes=VMEM),
        cost_estimate=pl.CostEstimate(flops=flops, bytes_accessed=4 * d * tokens, transcendentals=0),
        name="layer_forward",
    )(a, wg, wu, wd)


def backward_kernel(a, dh, wg, wu, wd, da, gu_out, d_out,
                    acc, wt, wgu, hid, dgu, gu, dd,
                    sa_gu, sa_d, ra_gu, ra_d, ka_gu, ka_d,
                    sb_gu, sb_d, rb_gu, rb_d, kb_gu, kb_d,
                    sc_gu, sc_d, rc_gu, rc_d, o_gu, o_d,
                    send, recv, out_sem):
    step = pl.program_id(0)
    me = lax.axis_index("dp")
    core, z0, z1 = me % 2, (me // 2) % 2, me // 4
    partners = (me + 1 - 2 * core, me + 2 - 4 * z0, me + 4 - 8 * z1)
    d, tokens = a.shape
    c = hid.shape[0]

    @pl.when(step == 0)
    def _():
        barrier = pltpu.get_barrier_semaphore()
        for p in partners:
            pl.semaphore_signal(barrier, 1, device_id={"dp": p}, device_id_type=MESH)
        pl.semaphore_wait(barrier, 3)
        acc[...] = jnp.zeros_like(acc)

    def copies(stage, slot):
        pairs = (((sa_gu, ra_gu), (sa_d, ra_d)), ((sb_gu, rb_gu), (sb_d, rb_d)), ((sc_gu, rc_gu), (sc_d, rc_d)))[stage]
        return [
            pltpu.make_async_remote_copy(
                src_ref=s, dst_ref=r.at[slot], send_sem=send.at[stage, n], recv_sem=recv.at[stage, n, slot],
                device_id={"dp": partners[stage]}, device_id_type=MESH)
            for n, (s, r) in enumerate(pairs)
        ]

    def outs(chunk):
        return [pltpu.make_async_copy(o_gu, gu_out.at[chunk], out_sem.at[0]),
                pltpu.make_async_copy(o_d, d_out.at[chunk], out_sem.at[1])]

    @pl.when(step < NC)
    def _():
        wt[:c] = wg[0].T
        wt[c:] = wu[0].T
        wgu[:, :c] = wg[0]
        wgu[:, c:] = wu[0]

        def body(t, _):
            for k in range(2):
                at = pl.ds(pl.multiple_of((2 * t + k) * TILE, TILE), TILE)
                x = a[:, at]
                gate, up = dot(wt[:c], x), dot(wt[c:], x)
                by_hid = dot(wd[0].reshape(c, d), dh[:, at]).astype(BF16).astype(F32)
                sig = sigmoid(gate)
                silu = gate * sig
                hid[:, at] = (silu * up).astype(BF16)
                dgu[:c, at] = (by_hid * up * (sig + silu * (1.0 - sig))).astype(BF16)
                dgu[c:, at] = (by_hid * silu).astype(BF16)
            return 0

        lax.fori_loop(0, tokens // TILE // 2, body, 0)

    @pl.when(step >= 4)
    def _():
        for copy in outs(step - 4):
            copy.wait()

    @pl.when(step >= 3)
    def _():
        slot = (step - 3) % 2
        for copy in copies(2, slot):
            copy.wait()
        o_gu[...] = (kb_gu[z1] + rc_gu[slot].astype(F32)).astype(BF16)
        o_d[...] = (kb_d[z1] + rc_d[slot].astype(F32)).astype(BF16)
        for copy in outs(step - 3):
            copy.start()

    @pl.when((step >= 2) & (step < NC + 2))
    def _():
        slot = (step - 2) % 2
        for copy in copies(1, slot):
            copy.wait()
        for half in range(2):
            kb_gu[half] = ka_gu[half, z0] + rb_gu[slot, half].astype(F32)
            kb_d[half] = ka_d[half, z0] + rb_d[slot, half].astype(F32)
        sc_gu[...] = kb_gu[1 - z1].astype(BF16)
        sc_d[...] = kb_d[1 - z1].astype(BF16)
        for copy in copies(2, slot):
            copy.start()

    @pl.when((step >= 1) & (step < NC + 1))
    def _():
        slot = (step - 1) % 2
        for copy in copies(0, slot):
            copy.wait()
        for i in range(2):
            for j in range(2):
                ka_gu[i, j] = gu[i, j, core] + ra_gu[slot, i, j].astype(F32)
                ka_d[i, j] = dd[i, j, core] + ra_d[slot, i, j].astype(F32)
            sb_gu[i] = ka_gu[i, 1 - z0].astype(BF16)
            sb_d[i] = ka_d[i, 1 - z0].astype(BF16)
        for copy in copies(1, slot):
            copy.start()

    @pl.when(step < NC)
    def _():
        def body(t, _):
            at = pl.ds(pl.multiple_of(t * WIDE, WIDE), WIDE)
            g = dgu[:, at]
            acc[:, at] += dot(wgu[...], g)
            return 0

        lax.fori_loop(0, tokens // WIDE, body, 0)

        shape = gu.shape
        gu[...] = dot_nt(a[...], dgu[...]).reshape(shape)
        dd[...] = dot_nt(dh[...], hid[...]).T.reshape(dd.shape)
        for i in range(2):
            for j in range(2):
                sa_gu[i, j] = gu[i, j, 1 - core].astype(BF16)
                sa_d[i, j] = dd[i, j, 1 - core].astype(BF16)
        for copy in copies(0, step % 2):
            copy.start()

    @pl.when(step == NC - 1)
    def _():
        da[...] = acc[...].astype(BF16)

    @pl.when(step == NC + 2)
    def _():
        for copy in outs(NC - 1):
            copy.wait()


def backward(a, dh, wg, wu, wd, number):
    d, tokens = a.shape
    c = wg.shape[2] // 2
    m, n = d // 8, c // 8
    whole = pl.BlockSpec((d, tokens), lambda s: (0, 0), pipeline_mode=pl.Buffered(1))
    anywhere = pl.BlockSpec(memory_space=pl.ANY)
    both = lambda *lead, dtype: [pltpu.VMEM((*lead, m, 2 * c), dtype), pltpu.VMEM((*lead, n, d), dtype)]
    return pl.pallas_call(
        backward_kernel,
        grid=(NC + 3,),
        out_shape=[
            jax.ShapeDtypeStruct((d, tokens), BF16),
            jax.ShapeDtypeStruct((NC, m, 2 * c), BF16),
            jax.ShapeDtypeStruct((NC, n, d), BF16),
        ],
        in_specs=[whole, whole, *weight_specs(d, c)],
        out_specs=[whole, anywhere, anywhere],
        scratch_shapes=[
            pltpu.VMEM((d, tokens), F32),
            pltpu.VMEM((2 * c, d), BF16),
            pltpu.VMEM((d, 2 * c), BF16),
            pltpu.VMEM((c, tokens), BF16),
            pltpu.VMEM((2 * c, tokens), BF16),
            *both(2, 2, 2, dtype=F32),
            *both(2, 2, dtype=BF16), *both(2, 2, 2, dtype=BF16), *both(2, 2, dtype=F32),
            *both(2, dtype=BF16), *both(2, 2, dtype=BF16), *both(2, dtype=F32),
            *both(dtype=BF16), *both(2, dtype=BF16), *both(dtype=BF16),
            pltpu.SemaphoreType.DMA((3, 2)),
            pltpu.SemaphoreType.DMA((3, 2, 2)),
            pltpu.SemaphoreType.DMA((2,)),
        ],
        compiler_params=pltpu.CompilerParams(vmem_limit_bytes=VMEM, collective_id=1 + number, has_side_effects=True),
        cost_estimate=pl.CostEstimate(flops=16 * d * tokens * c * NC, bytes_accessed=6 * d * tokens, transcendentals=0),
        name=f"layer_backward_{number}",
    )(a, dh, wg, wu, wd)


def gather_kernel(cols, rows, cols_all, rows_all, send, recv, local):
    me, rep = lax.axis_index("dp"), lax.axis_index("rep")
    core, z0, z1 = me % 2, (me // 2) % 2, me // 4
    x, y = rep // 2, rep % 2
    sibling, near, far = me + 1 - 2 * core, me + 2 - 4 * z0, me + 4 - 8 * z1
    both = far + 2 - 4 * z0
    by_x, by_y = rep + 2 - 4 * x, rep + 1 - 2 * y
    q, r = cols.shape[-1] // 4, rows.shape[-2] // 4

    barrier = pltpu.get_barrier_semaphore()
    peers = [{"dp": far}, {"dp": near}, {"rep": by_x}, {"rep": by_y}, {"dp": sibling}]
    for p in peers:
        pl.semaphore_signal(barrier, 1, device_id=p, device_id_type=MESH)
    pl.semaphore_wait(barrier, len(peers))

    mine = []
    for i in range(4):
        mine.append(pltpu.make_async_copy(cols.at[i], cols_all.at[i, :, me], local.at[i]))
    for i in range(2):
        mine.append(pltpu.make_async_copy(rows.at[i], rows_all.at[i, :, me], local.at[4 + i]))
    for copy in mine:
        copy.start()

    pieces = []
    for layer in range(2):
        pieces += [("c", 2 * layer), ("c", 2 * layer + 1), ("r", layer)]

    def part(piece, owner, quarter):
        kind, i = pieces[piece]
        if kind == "c":
            return cols_all.at[i, :, owner, :, pl.ds(pl.multiple_of(quarter * q, q), q)]
        return rows_all.at[i, :, owner, pl.ds(pl.multiple_of(quarter * r, r), r), :]

    def first(piece):
        kind, i = pieces[piece]
        if kind == "c":
            return cols.at[i, :, :, pl.ds(pl.multiple_of(rep * q, q), q)]
        return rows.at[i, :, pl.ds(pl.multiple_of(rep * r, r), r), :]

    def shard(piece, owner):
        kind, i = pieces[piece]
        return cols_all.at[i, :, owner] if kind == "c" else rows_all.at[i, :, owner]

    def stage(piece, s):
        flip = piece in (1, 3, 5)
        one, two = (by_y, by_x) if flip else (by_x, by_y)
        if s == 0:
            return [(first(piece), part(piece, me, rep), {"dp": far}, 0)]
        if s == 1:
            return [(first(piece), part(piece, me, rep), {"dp": near}, 1),
                    (part(piece, far, rep), part(piece, far, rep), {"dp": near}, 2)]
        if s == 2:
            return [(part(piece, o, rep), part(piece, o, rep), {"rep": one}, 3 + n) for n, o in enumerate((far, near, both))]
        if s == 3:
            return [(part(piece, o, w), part(piece, o, w), {"rep": two}, 6 + 2 * n + k)
                    for n, o in enumerate((far, near, both)) for k, w in enumerate((rep, one))]
        own = [(shard(piece, o), shard(piece, o), {"dp": sibling}, 13 + n) for n, o in enumerate((far, near, both))]
        kind, i = pieces[piece]
        src = cols.at[i] if kind == "c" else rows.at[i]
        return [(src, shard(piece, me), {"dp": sibling}, 12)] + own

    def copies(piece, s):
        return [pltpu.make_async_remote_copy(src_ref=a, dst_ref=b, send_sem=send.at[piece, n], recv_sem=recv.at[piece, n],
                                             device_id=dev, device_id_type=MESH) for a, b, dev, n in stage(piece, s)]

    count = len(pieces)
    for wave in range(count + 5):
        for s in reversed(range(5)):
            piece = wave - s
            if 0 <= piece < count:
                if s:
                    for copy in copies(piece, s - 1):
                        copy.wait_recv()
                for copy in copies(piece, s):
                    copy.start()
        piece = wave - 5
        if 0 <= piece < count:
            for copy in copies(piece, 4):
                copy.wait_recv()
    for piece in range(count):
        for s in range(5):
            for copy in copies(piece, s):
                copy.wait_send()
    for copy in mine:
        copy.wait()


def gather(cols, rows):
    inside = pl.BlockSpec(memory_space=pltpu.VMEM)
    anywhere = pl.BlockSpec(memory_space=pl.ANY)
    return pl.pallas_call(
        gather_kernel,
        out_shape=[
            jax.ShapeDtypeStruct((*cols.shape[:2], 8, *cols.shape[2:]), BF16),
            jax.ShapeDtypeStruct((*rows.shape[:2], 8, *rows.shape[2:]), BF16),
        ],
        in_specs=[inside, inside],
        out_specs=[anywhere, anywhere],
        scratch_shapes=[pltpu.SemaphoreType.DMA((6, 16)), pltpu.SemaphoreType.DMA((6, 16)), pltpu.SemaphoreType.DMA((6,))],
        compiler_params=pltpu.CompilerParams(collective_id=0, has_side_effects=True, vmem_limit_bytes=VMEM),
        cost_estimate=pl.CostEstimate(flops=10**11, bytes_accessed=6 * 10**7, transcendentals=0),
        name="gather_weights",
    )(cols, rows)


def scale_of(h):
    wide = h.astype(F32)
    return lax.rsqrt(jnp.mean(wide**2, 0, keepdims=True) + 1e-6)


def normed(h):
    return (h.astype(F32) * scale_of(h)).astype(BF16)


def through_norm(h, by_a, by_h):
    wide, g, scale = h.astype(F32), by_a.astype(F32), scale_of(h)
    back = g * scale - wide * (scale**3 * jnp.mean(g * wide, 0, keepdims=True))
    return (by_h.astype(F32) + back.astype(BF16).astype(F32)).astype(BF16)


def solution(mesh):
    def local(x, dy, wg, wu, wd):
        layers, m, ff = wg.shape
        d = wd.shape[2]
        n = wd.shape[1] // NC
        h0, by_y = x[0].T, dy[0].T

        def ordered(w):
            w = w.reshape(layers, m, 8, NC // 2, 2, n).transpose(0, 3, 1, 4, 2, 5)
            return w.reshape(layers, NC // 2, m, 16 * n)

        cols = jnp.stack([ordered(wg), ordered(wu)], 1).reshape(2 * layers, NC // 2, m, 16 * n)
        rows = wd.reshape(layers, NC // 2, 2 * n, d)
        cols, rows = gather(cols, rows)
        cols = cols.reshape(layers, 2, NC // 2, d, 16 * n)
        weights = [(cols[i, 0], cols[i, 1], rows[i]) for i in range(layers)]

        a0 = normed(h0)
        h1 = (h0.astype(F32) + forward(a0, *weights[0]).astype(F32)).astype(BF16)
        a1 = normed(h1)
        by_a1, gu1, d1 = backward(a1, by_y, *weights[1], 1)
        by_h1 = through_norm(h1, by_a1, by_y)
        by_a0, gu0, d0 = backward(a0, by_h1, *weights[0], 0)
        by_x = through_norm(h0, by_a0, by_h1).T[None]

        def restored(*both):
            w = jnp.stack(both).reshape(layers, NC, m, 8, n).transpose(0, 2, 3, 1, 4)
            return w.reshape(layers, m, ff)

        half = 8 * n
        return (by_x, restored(gu0[..., :half], gu1[..., :half]), restored(gu0[..., half:], gu1[..., half:]),
                jnp.stack([d0, d1]).reshape(layers, NC * n, d))

    seq = P(("rep", "dp"), None, None)
    w = P(None, "dp", None)
    g = P("rep", "dp", None)
    return jax.shard_map(local, mesh=mesh, in_specs=(seq, seq, w, w, w), out_specs=(seq, g, g, g), check_vma=False)
```

```python
import functools

import jax
import jax.numpy as jnp
from jax import lax
from jax.experimental import pallas as pl
from jax.experimental.pallas import tpu as pltpu
from jax.sharding import PartitionSpec as P

MESH = pl.DeviceIdType.MESH
F32, BF16 = jnp.float32, jnp.bfloat16
NC = 10
VMEM = 67_000_000
TILE = 1024
WIDE = 2048


def dot(a, b):
    return jnp.dot(a, b, preferred_element_type=F32)


def dot_nt(a, b):
    return lax.dot_general(a, b, (((1,), (1,)), ((), ())), preferred_element_type=F32)


def sigmoid(x):
    return 0.5 * jnp.tanh(0.5 * x) + 0.5


def scale_of(wide):
    return lax.rsqrt(jnp.mean(wide * wide, 0, keepdims=True) + 1e-6)


PIECES, STAGES, SPACE = NC, 5, 2
WAVES = PIECES + SPACE * STAGES


class Gather:
    def __init__(self, cols, rows, cols_all, rows_all, send, recv, local):
        self.refs = cols, rows, cols_all, rows_all
        self.sems = send, recv, local
        me, rep = lax.axis_index("dp"), lax.axis_index("rep")
        core, z0, z1 = me % 2, (me // 2) % 2, me // 4
        x, y = rep // 2, rep % 2
        self.me, self.rep = me, rep
        self.sibling, self.near, self.far = me + 1 - 2 * core, me + 2 - 4 * z0, me + 4 - 8 * z1
        self.others = self.far, self.near, self.far + 2 - 4 * z0
        self.by_x, self.by_y = rep + 2 - 4 * x, rep + 1 - 2 * y

    def greet(self):
        barrier = pltpu.get_barrier_semaphore()
        peers = [{"dp": self.far}, {"dp": self.near}, {"rep": self.by_x}, {"rep": self.by_y}, {"dp": self.sibling}]
        for p in peers:
            pl.semaphore_signal(barrier, 1, device_id=p, device_id_type=MESH)
        pl.semaphore_wait(barrier, len(peers))

    def place(self):
        cols, rows, cols_all, rows_all = self.refs
        return [pltpu.make_async_copy(cols, cols_all.at[:, :, self.me], self.sems[2].at[0]),
                pltpu.make_async_copy(rows, rows_all.at[:, self.me], self.sems[2].at[1])]

    def own(self, piece, quarter=None):
        cols, rows = self.refs[:2]
        i = piece // 2
        if piece % 2 == 0:
            q = cols.shape[-1] // 4
            return cols.at[:, i] if quarter is None else cols.at[:, i, :, pl.ds(pl.multiple_of(quarter * q, q), q)]
        r = rows.shape[-2] // 4
        return rows.at[i] if quarter is None else rows.at[i, pl.ds(pl.multiple_of(quarter * r, r), r), :]

    def part(self, piece, owner, quarter=None):
        cols, rows = self.refs[2:]
        i = piece // 2
        if piece % 2 == 0:
            q = cols.shape[-1] // 4
            if quarter is None:
                return cols.at[:, i, owner]
            return cols.at[:, i, owner, :, pl.ds(pl.multiple_of(quarter * q, q), q)]
        r = rows.shape[-2] // 4
        if quarter is None:
            return rows.at[i, owner]
        return rows.at[i, owner, pl.ds(pl.multiple_of(quarter * r, r), r), :]

    def copies(self, piece, s):
        me, rep = self.me, self.rep
        flip = (piece // 2 + piece) % 2
        one, two = (self.by_y, self.by_x) if flip else (self.by_x, self.by_y)
        far, near, _ = self.others
        if s == 0:
            moves = [(self.own(piece, rep), self.part(piece, me, rep), {"dp": far}, 0)]
        elif s == 1:
            moves = [(self.own(piece, rep), self.part(piece, me, rep), {"dp": near}, 1),
                     (self.part(piece, far, rep), self.part(piece, far, rep), {"dp": near}, 2)]
        elif s == 2:
            moves = [(self.part(piece, o, rep), self.part(piece, o, rep), {"rep": one}, 3 + n) for n, o in enumerate(self.others)]
        elif s == 3:
            moves = [(self.part(piece, o, w), self.part(piece, o, w), {"rep": two}, 6 + 2 * n + k)
                     for n, o in enumerate(self.others) for k, w in enumerate((rep, one))]
        else:
            moves = [(self.own(piece), self.part(piece, me), {"dp": self.sibling}, 12)]
            moves += [(self.part(piece, o), self.part(piece, o), {"dp": self.sibling}, 13 + n) for n, o in enumerate(self.others)]
        send, recv, _ = self.sems
        return [pltpu.make_async_remote_copy(src_ref=a, dst_ref=b, send_sem=send.at[piece, n], recv_sem=recv.at[piece, n],
                                             device_id=dev, device_id_type=MESH) for a, b, dev, n in moves]

    def wave(self, w):
        if w == 0:
            self.greet()
            for copy in self.place():
                copy.start()
        for s in reversed(range(STAGES + 1)):
            piece = w - SPACE * s
            if 0 <= piece < PIECES:
                if s:
                    for copy in self.copies(piece, s - 1):
                        copy.wait_recv()
                if s < STAGES:
                    for copy in self.copies(piece, s):
                        copy.start()
        if w == WAVES - 1:
            for piece in range(PIECES):
                for s in range(STAGES):
                    for copy in self.copies(piece, s):
                        copy.wait_send()
            for copy in self.place():
                copy.wait()


def gather_io(cols, rows):
    anywhere = pl.BlockSpec(memory_space=pl.ANY)
    inside = [pl.BlockSpec(t.shape, lambda s, n=t.ndim: (0,) * n, pipeline_mode=pl.Buffered(1)) for t in (cols, rows)]
    shapes = [jax.ShapeDtypeStruct((2, NC // 2, 8, *cols.shape[2:]), BF16), jax.ShapeDtypeStruct((NC // 2, 8, *rows.shape[1:]), BF16)]
    sems = [pltpu.SemaphoreType.DMA((PIECES, 16)), pltpu.SemaphoreType.DMA((PIECES, 16)), pltpu.SemaphoreType.DMA((2,))]
    return inside, [anywhere, anywhere], shapes, sems


FIRST = 16


def first_kernel(cols, rows, x, dy, cols_all, rows_all, h, a, by_y, send, recv, local):
    step = pl.program_id(0)
    gather = Gather(cols, rows, cols_all, rows_all, send, recv, local)
    for w in range(WAVES):
        pl.when(step == w)(functools.partial(gather.wave, w))

    @pl.when(step < FIRST)
    def _():
        turned = x[...].T
        h[...] = turned
        wide = turned.astype(F32)
        a[...] = (wide * scale_of(wide)).astype(BF16)
        by_y[...] = dy[...].T


def first(cols, rows, x, dy):
    tokens, d = x.shape
    size = tokens // FIRST
    inside, anywhere, shapes, sems = gather_io(cols, rows)
    tall = pl.BlockSpec((size, d), lambda s: (jnp.minimum(s, FIRST - 1), 0))
    wide = pl.BlockSpec((d, size), lambda s: (0, jnp.minimum(s, FIRST - 1)))
    state = jax.ShapeDtypeStruct((d, tokens), BF16)
    return pl.pallas_call(
        first_kernel,
        grid=(WAVES,),
        out_shape=[*shapes, state, state, state],
        in_specs=[*inside, tall, tall],
        out_specs=[*anywhere, wide, wide, wide],
        scratch_shapes=sems,
        compiler_params=pltpu.CompilerParams(collective_id=0, has_side_effects=True, vmem_limit_bytes=VMEM),
        cost_estimate=pl.CostEstimate(flops=10**11, bytes_accessed=6 * 10**7, transcendentals=0),
        name="gather_first",
    )(cols, rows, x, dy)


def forward_kernel(a, h, wg, wu, wd, cols, rows, h_out, a_out, cols_all, rows_all, acc, wgt, wut, wdt, send, recv, local):
    step = pl.program_id(0)
    c = wgt.shape[0]
    d, tokens = a.shape
    gather = Gather(cols, rows, cols_all, rows_all, send, recv, local)

    def waves(i):
        gather.wave(2 * i)
        gather.wave(2 * i + 1)

    for i in range(NC):
        pl.when(step == i)(functools.partial(waves, i))

    wgt[...] = wg[0, 0].T
    wut[...] = wu[0, 0].T
    wdt[...] = wd[0].reshape(c, d).T

    @pl.when(step == 0)
    def _():
        acc[...] = jnp.zeros_like(acc)

    def body(t, _):
        for k in range(2):
            at = pl.ds(pl.multiple_of((2 * t + k) * TILE, TILE), TILE)
            x = a[:, at]
            gate, up = dot(wgt[...], x), dot(wut[...], x)
            hid = (gate * sigmoid(gate) * up).astype(BF16)
            acc[:, at] += dot(wdt[...], hid)
        return 0

    lax.fori_loop(0, tokens // TILE // 2, body, 0)

    @pl.when(step == NC - 1)
    def _():
        def finish(t, _):
            at = pl.ds(pl.multiple_of(t * 256, 256), 256)
            out = (h[:, at].astype(F32) + acc[:, at].astype(BF16).astype(F32)).astype(BF16)
            h_out[:, at] = out
            wide = out.astype(F32)
            a_out[:, at] = (wide * scale_of(wide)).astype(BF16)
            return 0

        lax.fori_loop(0, tokens // 256, finish, 0)


def weight_specs(d, c):
    at = lambda s: jnp.minimum(s, NC - 1)
    gate = pl.BlockSpec((1, 1, d, c), lambda s: (0, at(s) // 2, 0, at(s) % 2))
    up = pl.BlockSpec((1, 1, d, c), lambda s: (1, at(s) // 2, 0, at(s) % 2))
    down = pl.BlockSpec((1, 8, c // 8, d), lambda s: (at(s) // 2, 0, at(s) % 2, 0))
    return [gate, up, down]


def forward(a, h, w, wd, cols, rows):
    d, tokens = a.shape
    c = w.shape[3] // 2
    whole = pl.BlockSpec((d, tokens), lambda s: (0, 0), pipeline_mode=pl.Buffered(1))
    state = jax.ShapeDtypeStruct((d, tokens), BF16)
    inside, anywhere, shapes, sems = gather_io(cols, rows)
    assert WAVES == 2 * NC
    return pl.pallas_call(
        forward_kernel,
        grid=(NC,),
        out_shape=[state, state, *shapes],
        in_specs=[whole, whole, *weight_specs(d, c), *inside],
        out_specs=[whole, whole, *anywhere],
        scratch_shapes=[
            pltpu.VMEM((d, tokens), F32),
            pltpu.VMEM((c, d), BF16),
            pltpu.VMEM((c, d), BF16),
            pltpu.VMEM((d, c), BF16),
            *sems,
        ],
        compiler_params=pltpu.CompilerParams(vmem_limit_bytes=VMEM, collective_id=3, has_side_effects=True),
        cost_estimate=pl.CostEstimate(flops=6 * d * tokens * c * NC, bytes_accessed=8 * d * tokens, transcendentals=0),
        name="layer_forward",
    )(a, h, w, w, wd, cols, rows)


def backward_kernel(a, dh, wg, wu, wd, h, out, gu_out, d_out,
                    acc, wt, wgu, hid, dgu, gu, dd,
                    sa_gu, sa_d, ra_gu, ra_d, ka_gu, ka_d,
                    sb_gu, sb_d, rb_gu, rb_d, kb_gu, kb_d,
                    sc_gu, sc_d, rc_gu, rc_d, o_gu, o_d,
                    send, recv, out_sem, h_sem):
    step = pl.program_id(0)
    me = lax.axis_index("dp")
    core, z0, z1 = me % 2, (me // 2) % 2, me // 4
    partners = (me + 1 - 2 * core, me + 2 - 4 * z0, me + 4 - 8 * z1)
    d, tokens = a.shape
    c = hid.shape[0]
    fetch = pltpu.make_async_copy(h, out, h_sem)

    @pl.when(step == 0)
    def _():
        fetch.start()
        barrier = pltpu.get_barrier_semaphore()
        for p in partners:
            pl.semaphore_signal(barrier, 1, device_id={"dp": p}, device_id_type=MESH)
        pl.semaphore_wait(barrier, 3)
        acc[...] = jnp.zeros_like(acc)

    def copies(stage, slot):
        pairs = (((sa_gu, ra_gu), (sa_d, ra_d)), ((sb_gu, rb_gu), (sb_d, rb_d)), ((sc_gu, rc_gu), (sc_d, rc_d)))[stage]
        return [
            pltpu.make_async_remote_copy(
                src_ref=s, dst_ref=r.at[slot], send_sem=send.at[stage, n], recv_sem=recv.at[stage, n, slot],
                device_id={"dp": partners[stage]}, device_id_type=MESH)
            for n, (s, r) in enumerate(pairs)
        ]

    def outs(chunk):
        return [pltpu.make_async_copy(o_gu, gu_out.at[chunk], out_sem.at[0]),
                pltpu.make_async_copy(o_d, d_out.at[chunk], out_sem.at[1])]

    @pl.when(step < NC)
    def _():
        wt[:c] = wg[0, 0].T
        wt[c:] = wu[0, 0].T
        wgu[:, :c] = wg[0, 0]
        wgu[:, c:] = wu[0, 0]

        def body(t, _):
            for k in range(2):
                at = pl.ds(pl.multiple_of((2 * t + k) * TILE, TILE), TILE)
                x = a[:, at]
                gate, up = dot(wt[:c], x), dot(wt[c:], x)
                by_hid = dot(wd[0].reshape(c, d), dh[:, at]).astype(BF16).astype(F32)
                sig = sigmoid(gate)
                silu = gate * sig
                hid[:, at] = (silu * up).astype(BF16)
                dgu[:c, at] = (by_hid * up * (sig + silu * (1.0 - sig))).astype(BF16)
                dgu[c:, at] = (by_hid * silu).astype(BF16)
            return 0

        lax.fori_loop(0, tokens // TILE // 2, body, 0)

    @pl.when(step == NC)
    def _():
        fetch.wait()

        def finish(t, _):
            at = pl.ds(pl.multiple_of(t * 256, 256), 256)
            wide, g = out[:, at].astype(F32), acc[:, at].astype(BF16).astype(F32)
            scale = scale_of(wide)
            through = g * scale - wide * (scale**3 * jnp.mean(g * wide, 0, keepdims=True))
            out[:, at] = (dh[:, at].astype(F32) + through.astype(BF16).astype(F32)).astype(BF16)
            return 0

        lax.fori_loop(0, tokens // 256, finish, 0)

    @pl.when(step >= 4)
    def _():
        for copy in outs(step - 4):
            copy.wait()

    @pl.when(step >= 3)
    def _():
        slot = (step - 3) % 2
        for copy in copies(2, slot):
            copy.wait()
        o_gu[...] = (kb_gu[z1] + rc_gu[slot].astype(F32)).astype(BF16)
        o_d[...] = (kb_d[z1] + rc_d[slot].astype(F32)).astype(BF16)
        for copy in outs(step - 3):
            copy.start()

    @pl.when((step >= 2) & (step < NC + 2))
    def _():
        slot = (step - 2) % 2
        for copy in copies(1, slot):
            copy.wait()
        for half in range(2):
            kb_gu[half] = ka_gu[half, z0] + rb_gu[slot, half].astype(F32)
            kb_d[half] = ka_d[half, z0] + rb_d[slot, half].astype(F32)
        sc_gu[...] = kb_gu[1 - z1].astype(BF16)
        sc_d[...] = kb_d[1 - z1].astype(BF16)
        for copy in copies(2, slot):
            copy.start()

    @pl.when((step >= 1) & (step < NC + 1))
    def _():
        slot = (step - 1) % 2
        for copy in copies(0, slot):
            copy.wait()
        for i in range(2):
            for j in range(2):
                ka_gu[i, j] = gu[i, j, core] + ra_gu[slot, i, j].astype(F32)
                ka_d[i, j] = dd[i, j, core] + ra_d[slot, i, j].astype(F32)
            sb_gu[i] = ka_gu[i, 1 - z0].astype(BF16)
            sb_d[i] = ka_d[i, 1 - z0].astype(BF16)
        for copy in copies(1, slot):
            copy.start()

    @pl.when(step < NC)
    def _():
        def body(t, _):
            at = pl.ds(pl.multiple_of(t * WIDE, WIDE), WIDE)
            g = dgu[:, at]
            acc[:, at] += dot(wgu[...], g)
            return 0

        lax.fori_loop(0, tokens // WIDE, body, 0)

        shape = gu.shape
        gu[...] = dot_nt(a[...], dgu[...]).reshape(shape)
        dd[...] = dot_nt(dh[...], hid[...]).T.reshape(dd.shape)
        for i in range(2):
            for j in range(2):
                sa_gu[i, j] = gu[i, j, 1 - core].astype(BF16)
                sa_d[i, j] = dd[i, j, 1 - core].astype(BF16)
        for copy in copies(0, step % 2):
            copy.start()

    @pl.when(step == NC + 2)
    def _():
        for copy in outs(NC - 1):
            copy.wait()


def backward(a, dh, h, w, wd, number):
    d, tokens = a.shape
    c = w.shape[3] // 2
    m, n = d // 8, c // 8
    whole = pl.BlockSpec((d, tokens), lambda s: (0, 0), pipeline_mode=pl.Buffered(1))
    anywhere = pl.BlockSpec(memory_space=pl.ANY)
    both = lambda *lead, dtype: [pltpu.VMEM((*lead, m, 2 * c), dtype), pltpu.VMEM((*lead, n, d), dtype)]
    return pl.pallas_call(
        backward_kernel,
        grid=(NC + 3,),
        out_shape=[
            jax.ShapeDtypeStruct((d, tokens), BF16),
            jax.ShapeDtypeStruct((NC, m, 2 * c), BF16),
            jax.ShapeDtypeStruct((NC, n, d), BF16),
        ],
        in_specs=[whole, whole, *weight_specs(d, c), anywhere],
        out_specs=[whole, anywhere, anywhere],
        scratch_shapes=[
            pltpu.VMEM((d, tokens), F32),
            pltpu.VMEM((2 * c, d), BF16),
            pltpu.VMEM((d, 2 * c), BF16),
            pltpu.VMEM((c, tokens), BF16),
            pltpu.VMEM((2 * c, tokens), BF16),
            *both(2, 2, 2, dtype=F32),
            *both(2, 2, dtype=BF16), *both(2, 2, 2, dtype=BF16), *both(2, 2, dtype=F32),
            *both(2, dtype=BF16), *both(2, 2, dtype=BF16), *both(2, dtype=F32),
            *both(dtype=BF16), *both(2, dtype=BF16), *both(dtype=BF16),
            pltpu.SemaphoreType.DMA((3, 2)),
            pltpu.SemaphoreType.DMA((3, 2, 2)),
            pltpu.SemaphoreType.DMA((2,)),
            pltpu.SemaphoreType.DMA,
        ],
        compiler_params=pltpu.CompilerParams(vmem_limit_bytes=VMEM, collective_id=1 + number, has_side_effects=True),
        cost_estimate=pl.CostEstimate(flops=16 * d * tokens * c * NC, bytes_accessed=6 * d * tokens, transcendentals=0),
        name=f"layer_backward_{number}",
    )(a, dh, w, w, wd, h)


def solution(mesh):
    def local(x, dy, wg, wu, wd):
        layers, m, ff = wg.shape
        d = wd.shape[2]
        n = wd.shape[1] // NC

        def ordered(w):
            w = w.reshape(layers, m, 8, NC // 2, 2, n).transpose(0, 3, 1, 4, 2, 5)
            return w.reshape(layers, NC // 2, m, 16 * n)

        cols = jnp.stack([ordered(wg), ordered(wu)], 1)
        rows = wd.reshape(layers, NC // 2, 2 * n, d)
        together = lambda w: w.reshape(2, NC // 2, d, 16 * n)
        w0, wd0, h0, a0, by_y = first(cols[0], rows[0], x[0], dy[0])
        w0 = together(w0)
        h1, a1, w1, wd1 = forward(a0, h0, w0, wd0, cols[1], rows[1])
        by_h1, gu1, d1 = backward(a1, by_y, h1, together(w1), wd1, 1)
        by_h0, gu0, d0 = backward(a0, by_h1, h0, w0, wd0, 0)
        by_x = by_h0.T[None]

        def restored(*both):
            w = jnp.stack(both).reshape(layers, NC, m, 8, n).transpose(0, 2, 3, 1, 4)
            return w.reshape(layers, m, ff)

        half = 8 * n
        return (by_x, restored(gu0[..., :half], gu1[..., :half]), restored(gu0[..., half:], gu1[..., half:]),
                jnp.stack([d0, d1]).reshape(layers, NC * n, d))

    seq = P(("rep", "dp"), None, None)
    w = P(None, "dp", None)
    g = P("rep", "dp", None)
    return jax.shard_map(local, mesh=mesh, in_specs=(seq, seq, w, w, w), out_specs=(seq, g, g, g), check_vma=False)
```
